32 devices in a mesh: space: 16 (over z, y, core), peer: 2 (over x).
Axes of the slice: x: 2, y: 2, z: 4, core: 2. Of those that a mesh axis runs over, the one named last changes fastest.
Arguments:
- wavefield: float32 [2, 9, 128, 64, 128], P('peer', None, 'space'), may hold values from -100 to 100
- buoyancy: float32 [128, 64, 128], P('space'), may hold values from 0.2 to 0.5
- lame_lambda: float32 [128, 64, 128], P('space'), may hold values from 0.06 to 0.12
- shear_modulus: float32 [128, 64, 128], P('space'), may hold values from 0.05 to 0.1
- scale_exponents: int32 [9, 16, 8, 16], P(None, 'space'), may hold values from -2 to 2
- source_cells: int32 [2, 8], replicated, may hold values from 0 to 1048575
- wavelet: float32 [2, 3, 8], replicated, may hold values from -18 to 18
Outputs:
- final_field: float32 [2, 9, 128, 64, 128], P('peer', None, 'space')
- stored: bfloat16 [2, 3, 9, 128, 64, 128], P('peer', None, None, 'space')
- statistics: float32 [2, 3, 2], P('peer')
The draws below stay inside these ranges and needn't reach their ends.
All inputs are finite; a program needn't handle non-finite values.
Results may differ from the reference program's by a relative error of at most 0.0045.
Values may be sent and summed in bfloat16 or wider, within the bound.
A program may use at most 64 MiB of HBM per device.

```python
import math
import jax
import jax.numpy as jnp
from jax import lax

NX = 128
NY = 64
BLOCK = 8
STEPS = 3
SRC = 8
SHOTS = 2
NZ = 128


def draw_wavefield(key, part):
    row_key, column_key, value_key = jax.random.split(key, 3)
    depth = jnp.arange(NZ, dtype=jnp.float32) / (NZ - 1)
    shape = (SHOTS, 9, NZ, NY, NX)
    ramp = 0.4 * jnp.exp(jnp.log(5.0) * depth)
    row_scale = jnp.exp(jax.random.uniform(row_key, (SHOTS, 1, 1, NY, 1), minval=jnp.log(0.32), maxval=jnp.log(3.2)))
    column_scale = jnp.exp(jax.random.uniform(column_key, (SHOTS, 1, 1, 1, NX), minval=jnp.log(0.32), maxval=jnp.log(3.2)))
    values = jax.random.truncated_normal(value_key, -4.0, 4.0, shape)
    return (values * ramp[None, None, :, None, None] * row_scale * column_scale).astype(jnp.float32)


def set_ends(drawn, stream_key, least, top_value):
    place = [jax.random.randint(jax.random.fold_in(stream_key, axis), (), 0, length) for axis, length in enumerate(drawn.shape)]
    longest = drawn.shape.index(max(drawn.shape))
    neighbour = place[:longest] + [(place[longest] + 1) % drawn.shape[longest]] + place[longest + 1:]
    return drawn.at[tuple(place)].set(least).at[tuple(neighbour)].set(top_value)


def block_scale(key, shape, shards, least, top_value):
    level = 1.0
    for dim, parts in shards:
        steps = jax.random.uniform(jax.random.fold_in(jax.random.fold_in(key, 6), dim), (parts,), jnp.float32, least / len(shards), top_value / len(shards))
        level = level * jnp.repeat(jnp.exp(steps), shape[dim] // parts).reshape((-1,) + (1,) * (len(shape) - 1 - dim))
    return level


def centred(rng, extent, spread, bound, kind=jnp.bfloat16):
    entries = spread * jax.random.normal(rng, extent, jnp.float32)
    return jnp.clip(entries, min=-bound, max=bound).astype(kind)


def setup_inputs(seed: int = 0) -> dict:
    key_list = jax.random.split(jax.random.key(seed), 8)
    wavefield = draw_wavefield(jax.random.fold_in(key_list[7], 71), 0)
    buoyancy = jnp.clip(jnp.exp(math.log(0.5) - 0.9162907 * jax.random.uniform(key_list[1], (NZ, NY, NX), jnp.float32) ** block_scale(key_list[1], (NZ, NY, NX), ((0, 16),), -0.2, 0.2)), 0.2, 0.5)
    lame_lambda = jnp.clip(jnp.exp(math.log(0.12) - 0.6931472 * jax.random.uniform(key_list[2], (NZ, NY, NX), jnp.float32) ** block_scale(key_list[2], (NZ, NY, NX), ((0, 16),), -0.2, 0.2)), 0.06, 0.12)
    shear_modulus = jnp.clip(jnp.exp(math.log(0.1) - 0.6931472 * jax.random.uniform(key_list[3], (NZ, NY, NX), jnp.float32) ** block_scale(key_list[3], (NZ, NY, NX), ((0, 16),), -0.2, 0.2)), 0.05, 0.1)
    scale_exponents = set_ends(jax.random.randint(key_list[4], (9, NZ // BLOCK, NY // BLOCK, NX // BLOCK), -2, 3), jax.random.fold_in(key_list[4], 1), -2, 2).astype(jnp.int32)
    source_cells = set_ends(jax.random.randint(key_list[5], (SHOTS, SRC), 0, NZ * NY * NX), jax.random.fold_in(key_list[5], 1), 0, (NZ * NY * NX) - 1).astype(jnp.int32)
    wavelet = centred(key_list[6], (SHOTS, STEPS, SRC), 3.0, 18.0, jnp.float32)
    return {"wavefield": wavefield, "buoyancy": buoyancy, "lame_lambda": lame_lambda, "shear_modulus": shear_modulus, "scale_exponents": scale_exponents, "source_cells": source_cells, "wavelet": wavelet}


stencil_reach = 2
stencil_weights = (9.0 / 8.0, -1.0 / 24.0)
clip_level = 4.0
energy_floor = 1e-06

def pad_along(values, dimension):
    widths = [(0, 0)] * values.ndim
    widths[dimension] = (stencil_reach, stencil_reach)
    return jnp.pad(values, widths)

def derivative(padded, dimension, forward):
    length = padded.shape[dimension] - 2 * stencil_reach
    summed = None
    for offset in range(1, stencil_reach + 1):
        weight = stencil_weights[offset - 1]
        if forward:
            above_at = stencil_reach + offset
            below_at = stencil_reach + 1 - offset
        else:
            above_at = stencil_reach + offset - 1
            below_at = stencil_reach - offset
        portion = weight * (lax.slice_in_dim(padded, above_at, above_at + length, axis=dimension) - lax.slice_in_dim(padded, below_at, below_at + length, axis=dimension))
        summed = portion if summed is None else summed + portion
    return summed

def differ(values, dimension, forward):
    return derivative(pad_along(values, dimension), dimension, forward)

def pad_depth(stack):
    return pad_along(stack, 2)

def advance(current, buoyancy, lame_lambda, shear_modulus, images, stress_padder, velocity_padder):
    velocity = [current[:, component] for component in range(3)]
    stress = [current[:, component] for component in range(3, 9)]
    depth_rims = stress_padder(current[:, 6:9])
    velocity[0] = velocity[0] + buoyancy * (differ(stress[0], 3, True) + differ(stress[2], 2, False) + derivative(depth_rims[:, 1], 1, False))
    velocity[1] = velocity[1] + buoyancy * (differ(stress[2], 3, False) + differ(stress[1], 2, True) + derivative(depth_rims[:, 2], 1, False))
    velocity[2] = velocity[2] + buoyancy * (differ(stress[4], 3, False) + differ(stress[5], 2, False) + derivative(depth_rims[:, 0], 1, True))
    depth_rims = velocity_padder(jnp.stack(velocity, axis=1))
    strain = [differ(velocity[0], 3, False), differ(velocity[1], 2, False), derivative(depth_rims[:, 2], 1, False)]
    dilation = strain[0] + strain[1] + strain[2]
    pressure = lame_lambda * dilation + images
    stress[0] = stress[0] + pressure + 2.0 * shear_modulus * strain[0]
    stress[1] = stress[1] + pressure + 2.0 * shear_modulus * strain[1]
    stress[3] = stress[3] + pressure + 2.0 * shear_modulus * strain[2]
    stress[2] = stress[2] + shear_modulus * (differ(velocity[0], 2, True) + differ(velocity[1], 3, True))
    stress[4] = stress[4] + shear_modulus * (derivative(depth_rims[:, 0], 1, True) + differ(velocity[2], 3, True))
    stress[5] = stress[5] + shear_modulus * (derivative(depth_rims[:, 1], 1, True) + differ(velocity[2], 2, True))
    return jnp.stack(velocity + stress, axis=1)

def scale_tables(exponents):
    expanded = jnp.repeat(jnp.repeat(jnp.repeat(exponents, BLOCK, axis=1), BLOCK, axis=2), BLOCK, axis=3)
    upscale = jnp.zeros(expanded.shape, jnp.float32)
    downscale = jnp.zeros(expanded.shape, jnp.float32)
    for exponent in range(-2, 3):
        chosen = expanded == exponent
        upscale = jnp.where(chosen, jnp.float32(2.0 ** exponent), upscale)
        downscale = jnp.where(chosen, jnp.float32(2.0 ** (-exponent)), downscale)
    return (upscale, downscale)

def compress(current, upscale, downscale):
    payload = jnp.clip(current * downscale, -clip_level, clip_level).astype(jnp.bfloat16)
    levels = lax.optimization_barrier(payload).astype(jnp.float32)
    return (payload, levels, levels * upscale)

def finish(sums, cell_count):
    mean_size = sums[..., 0] / cell_count
    relative = sums[..., 1] / cell_count / (sums[..., 2] / cell_count + energy_floor)
    return jnp.stack([mean_size, jnp.sqrt(relative)], axis=-1)

def place_sources(cell_index, amounts):
    flat = jnp.zeros((NZ * NY * NX,), jnp.float32).at[cell_index].add(amounts)
    return flat.reshape(NZ, NY, NX)

def reference(wavefield, buoyancy, lame_lambda, shear_modulus, scale_exponents, source_cells, wavelet):
    upscale, downscale = scale_tables(scale_exponents)
    cell_count = 9 * NZ * NY * NX
    current = wavefield
    stored_list = []
    sums_list = []
    for instant in range(STEPS):
        images = jnp.stack([place_sources(source_cells[shot_index], wavelet[shot_index, instant]) for shot_index in range(SHOTS)], axis=0)
        current = advance(current, buoyancy, lame_lambda, shear_modulus, images, pad_depth, pad_depth)
        payload, levels, restored = compress(current, upscale, downscale)
        stored_list.append(payload[::-1])
        misfit = current - restored
        sums_list.append(jnp.stack([lax.optimization_barrier(jnp.sum(jnp.abs(levels), axis=(1, 2, 3, 4))), lax.optimization_barrier(jnp.sum(misfit * misfit, axis=(1, 2, 3, 4))), lax.optimization_barrier(jnp.sum(current * current, axis=(1, 2, 3, 4)))], axis=-1))
    stored = jnp.stack(stored_list, axis=1)
    statistics = finish(jnp.stack(sums_list, axis=1), cell_count)
    return (current, stored, statistics)
```

```python
import functools

import jax
import jax.numpy as jnp
from jax import lax
from jax.experimental import pallas as pl
from jax.experimental.pallas import tpu as pltpu
from jax.sharding import PartitionSpec as P

BLOCK = 8
STEPS = 3
REACH = 2
W1, W2 = 9.0 / 8.0, -1.0 / 24.0
CLIP = 4.0
FLOOR = 1e-06
HALVES = 2 * STEPS
PAD = 8
ROWS = 16
LEVELS = 32700.0
TINY = 1e-30
MESH = pl.DeviceIdType.MESH

KINDS = {"stress": ((7, 8), (6,)), "velocity": ((2,), (0, 1))}
ARRIVAL = (6, 7, 8, 3, 5, 0, 4, 1, 2)


def rim_layers(kind, depth):
    back, ahead = KINDS[kind]
    up = [(c, depth - 2, -2) for c in back] + [(c, depth - 1, -1) for c in back + ahead]
    down = [(c, 0, depth) for c in back + ahead] + [(c, 1, depth + 1) for c in ahead]
    return up, down


def kernel(
    wave, buoy_in, lam_in, mu_in, exps, cells, wavelet,
    final, stored, sums,
    cur, buoy, lam, mu, up_t, down_t, tx, rx, unit_tx, unit_rx, pay, h_tx, h_rx,
    load_sem, par_sem, out_sem, pay_sem, s_send, s_recv, u_send, u_recv, h_send, h_recv,
):
    peer = lax.axis_index("peer")
    slab = lax.axis_index("space")
    count = lax.axis_size("space")
    depth, rows, cols = buoy.shape
    groups = rows // ROWS
    other = 1 - peer

    def body_of(shot, c):
        return cur.at[shot, c, pl.ds(REACH, depth), pl.ds(PAD, rows), :]

    loads = {}
    for c in ARRIVAL:
        loads[c] = pltpu.make_async_copy(wave.at[0, c], body_of(0, c), load_sem.at[c])
        loads[c].start()
    params = []
    for i, (src, dst) in enumerate(((buoy_in, buoy), (lam_in, lam), (mu_in, mu))):
        params.append(pltpu.make_async_copy(src, dst, par_sem.at[i]))
        params[-1].start()

    has_up = slab < count - 1
    has_down = slab > 0
    barrier = pltpu.get_barrier_semaphore()
    pl.semaphore_signal(barrier, inc=1, device_id={"peer": other}, device_id_type=MESH)

    @pl.when(has_up)
    def _():
        pl.semaphore_signal(barrier, inc=1, device_id={"space": slab + 1}, device_id_type=MESH)

    @pl.when(has_down)
    def _():
        pl.semaphore_signal(barrier, inc=1, device_id={"space": slab - 1}, device_id_type=MESH)

    edge_rows = jnp.zeros((PAD, cols), jnp.float32)
    edge_layer = jnp.zeros((rows, cols), jnp.float32)
    for shot in range(2):

        def clear(c, carry, shot=shot):
            for z in range(depth + 2 * REACH):
                cur[shot, c, z, pl.ds(0, PAD), :] = edge_rows
                cur[shot, c, z, pl.ds(PAD + rows, PAD), :] = edge_rows
            for z in (0, 1, depth + 2, depth + 3):
                cur[shot, c, z, pl.ds(PAD, rows), :] = edge_layer
            return carry

        lax.fori_loop(0, 9, clear, 0)

    neighbours = jnp.minimum(slab, 1) + jnp.minimum(count - 1 - slab, 1)
    pl.semaphore_wait(barrier, 1 + neighbours)

    def exchange(c):
        return pltpu.make_async_remote_copy(
            src_ref=tx.at[c], dst_ref=rx.at[c], send_sem=s_send.at[c], recv_sem=s_recv.at[c],
            device_id={"peer": other}, device_id_type=MESH,
        )

    def exchange_unit(c):
        return pltpu.make_async_remote_copy(
            src_ref=unit_tx.at[c], dst_ref=unit_rx.at[c], send_sem=u_send.at[c],
            recv_sem=u_recv.at[c], device_id={"peer": other}, device_id_type=MESH,
        )

    def halo(h, way, size):
        target = slab + 1 if way == 0 else slab - 1
        return pltpu.make_async_remote_copy(
            src_ref=h_tx.at[h, way, pl.ds(0, size)], dst_ref=h_rx.at[h, way, pl.ds(0, size)],
            send_sem=h_send.at[h, way], recv_sem=h_recv.at[h, way],
            device_id={"space": target}, device_id_type=MESH,
        )

    def send_rims(shot, kind, h):
        for way, layers in enumerate(rim_layers(kind, depth)):
            for i, (c, z, _) in enumerate(layers):
                h_tx[h, way, i] = cur[shot, c, REACH + z, pl.ds(PAD, rows), :].astype(jnp.bfloat16)

            @pl.when(has_up if way == 0 else has_down)
            def _():
                halo(h, way, len(layers)).start()

    def take_rims(shot, kind, h):
        for way, layers in enumerate(rim_layers(kind, depth)):

            @pl.when(has_down if way == 0 else has_up)
            def _():
                halo(h, way, len(layers)).wait_recv()
                for i, (c, _, z) in enumerate(layers):
                    cur[shot, c, REACH + z, pl.ds(PAD, rows), :] = h_rx[h, way, i].astype(
                        jnp.float32
                    )

    def finish_sends(kind, h):
        for way, layers in enumerate(rim_layers(kind, depth)):

            @pl.when(has_up if way == 0 else has_down)
            def _():
                halo(h, way, len(layers)).wait_send()

    lane = lax.broadcasted_iota(jnp.int32, (ROWS, cols), 1)
    row = lax.broadcasted_iota(jnp.int32, (ROWS, cols), 0)
    spot = row * cols + lane

    def shifted(f, k):
        moved = pltpu.roll(f, (-k) % cols, 1)
        keep = lane < cols - k if k > 0 else lane >= -k
        return jnp.where(keep, moved, 0.0)

    def along_x(f, ahead):
        if ahead:
            return W1 * (shifted(f, 1) - f) + W2 * (shifted(f, 2) - shifted(f, -1))
        return W1 * (f - shifted(f, -1)) + W2 * (shifted(f, 1) - shifted(f, -2))

    def reader(shot, z, g):
        base = PAD + g * ROWS

        def read(c, dz=0, dy=0):
            return cur[shot, c, z + (REACH + dz), pl.ds(base + dy, ROWS), :]

        def along_y(c, ahead):
            o = 1 if ahead else 0
            return W1 * (read(c, 0, o) - read(c, 0, o - 1)) + W2 * (
                read(c, 0, o + 1) - read(c, 0, o - 2)
            )

        def along_z(c, ahead):
            o = 1 if ahead else 0
            return W1 * (read(c, o) - read(c, o - 1)) + W2 * (read(c, o + 1) - read(c, o - 2))

        def write(c, value):
            cur[shot, c, z + REACH, pl.ds(base, ROWS), :] = value

        return read, along_y, along_z, write

    def velocity_layer(shot, z):
        for g in range(groups):
            read, along_y, along_z, write = reader(shot, z, g)
            b = buoy[z, pl.ds(g * ROWS, ROWS), :]
            write(0, read(0) + b * (along_x(read(3), True) + along_y(5, False) + along_z(7, False)))
            write(1, read(1) + b * (along_x(read(5), False) + along_y(4, True) + along_z(8, False)))
            write(2, read(2) + b * (along_x(read(7), False) + along_y(8, False) + along_z(6, True)))

    def stress_layer(shot, t, z, totals):
        shot_index = peer if shot == 0 else other
        for g in range(groups):
            read, along_y, along_z, write = reader(shot, z, g)
            part = pl.ds(g * ROWS, ROWS)
            vx, vy, vz = read(0), read(1), read(2)
            ex, ey, ez = along_x(vx, False), along_y(1, False), along_z(2, False)
            image = jnp.zeros((ROWS, cols), jnp.float32)
            start = ((slab * depth + z) * rows + g * ROWS) * cols
            for j in range(cells.shape[1]):
                image = image + jnp.where(
                    spot == cells[shot_index, j] - start, wavelet[shot_index, t, j], 0.0
                )
            m = mu[z, part, :]
            pressure = lam[z, part, :] * (ex + ey + ez) + image
            twice = 2.0 * m
            values = [
                vx, vy, vz,
                read(3) + pressure + twice * ex,
                read(4) + pressure + twice * ey,
                read(5) + m * (along_y(0, True) + along_x(vy, True)),
                read(6) + pressure + twice * ez,
                read(7) + m * (along_z(0, True) + along_x(vz, True)),
                read(8) + m * (along_z(1, True) + along_y(2, True)),
            ]
            for c in range(3, 9):
                write(c, values[c])
            for c in range(9):
                v = values[c]
                packed = jnp.clip(v * down_t[c, part, :], -CLIP, CLIP).astype(jnp.bfloat16)
                if shot == 1:
                    pay[t, c, z, part, :] = packed
                else:
                    level = packed.astype(jnp.float32)
                    miss = v - level * up_t[c, part, :]
                    totals = (
                        totals[0] + jnp.abs(level),
                        totals[1] + miss * miss,
                        totals[2] + v * v,
                    )
        return totals

    nothing = jnp.zeros((ROWS, cols), jnp.float32)

    def inner(k):
        return k + 2

    def outer(k):
        return jnp.where(k < 2, k, k + (depth - 4))

    def half(shot, i):
        t, h = i // 2, shot * HALVES + i
        kind = "stress" if i % 2 == 0 else "velocity"
        if i % 2 == 0:

            def run(place, size, totals):
                def step(k, carry):
                    velocity_layer(shot, place(k))
                    return carry

                lax.fori_loop(0, size, step, 0)
                return totals
        else:

            def run(place, size, totals):
                def step(k, carry):
                    return stress_layer(shot, t, place(k), carry)

                return lax.fori_loop(0, size, step, totals)

        totals = run(inner, depth - 4, (nothing,) * 3)
        take_rims(shot, kind, h)
        totals = run(outer, 4, totals)
        if i < HALVES - 1:
            send_rims(shot, "velocity" if i % 2 == 0 else "stress", h + 1)
        if i % 2 and shot == 0:
            for s in range(3):
                sums[t, s] = totals[s]
        if i % 2 and shot == 1:
            payload_out(t).start()

    def payload_out(t):
        return pltpu.make_async_copy(pay.at[t], stored.at[0, t], pay_sem.at[t])

    def field_out(c):
        return pltpu.make_async_copy(body_of(0, c), final.at[0, c], out_sem.at[c])

    def unpack(c):
        exchange_unit(c).wait_recv()
        exchange(c).wait_recv()
        unit = unit_rx[c]

        def step(z, carry):
            for g in range(groups):
                whole = rx[c, z, pl.ds(g * ROWS, ROWS), :].astype(jnp.int32)
                cur[1, c, z + REACH, pl.ds(PAD + g * ROWS, ROWS), :] = (
                    whole.astype(jnp.float32) * unit
                )
            return carry

        lax.fori_loop(0, depth, step, 0)

    for c in ARRIVAL:
        loads[c].wait()

        def largest(z, top, c=c):
            for g in range(groups):
                top = jnp.maximum(
                    top, jnp.abs(cur[0, c, z + REACH, pl.ds(PAD + g * ROWS, ROWS), :])
                )
            return top

        top = lax.fori_loop(0, depth, largest, jnp.full((ROWS, cols), TINY, jnp.float32))
        unit_tx[c] = top * (1.0 / LEVELS)
        inverse = LEVELS / top

        def pack(z, carry, c=c, inverse=inverse):
            for g in range(groups):
                value = cur[0, c, z + REACH, pl.ds(PAD + g * ROWS, ROWS), :] * inverse
                tx[c, z, pl.ds(g * ROWS, ROWS), :] = (
                    jnp.round(value).astype(jnp.int32).astype(jnp.int16)
                )
            return carry

        lax.fori_loop(0, depth, pack, 0)
        exchange_unit(c).start()
        exchange(c).start()
        if c == 8:
            send_rims(0, "stress", 0)

    bands, strips = exps.shape[1], exps.shape[2]
    spread_y = (
        lax.broadcasted_iota(jnp.int32, (rows, bands), 0) // BLOCK
        == lax.broadcasted_iota(jnp.int32, (rows, bands), 1)
    ).astype(jnp.float32)
    spread_x = (
        lax.broadcasted_iota(jnp.int32, (strips, cols), 1) // BLOCK
        == lax.broadcasted_iota(jnp.int32, (strips, cols), 0)
    ).astype(jnp.float32)
    for c in range(9):
        e = exps[c]
        for table, sign in ((up_t, 1), (down_t, -1)):
            scale = jnp.zeros(e.shape, jnp.float32)
            for power in range(-2, 3):
                scale = jnp.where(e == power, jnp.float32(2.0 ** (sign * power)), scale)
            wide = jnp.dot(scale, spread_x, preferred_element_type=jnp.float32)
            table[c] = jnp.dot(spread_y, wide, preferred_element_type=jnp.float32)

    for p in params:
        p.wait()
    half(0, 0)
    half(0, 1)
    half(0, 2)
    for c in ARRIVAL[:3]:
        unpack(c)
    send_rims(1, "stress", HALVES)
    half(0, 3)
    for c in ARRIVAL[3:]:
        unpack(c)
    half(1, 0)
    half(0, 4)
    half(1, 1)
    half(0, 5)
    for c in range(9):
        field_out(c).start()
    for i in range(2, HALVES):
        half(1, i)

    for c in ARRIVAL:
        exchange(c).wait_send()
        exchange_unit(c).wait_send()
    for shot in range(2):
        for i in range(HALVES):
            finish_sends("stress" if i % 2 == 0 else "velocity", shot * HALVES + i)
    for c in range(9):
        field_out(c).wait()
    for t in range(STEPS):
        payload_out(t).wait()


def per_device(wavefield, buoyancy, lame_lambda, shear_modulus, exponents, cells, wavelet):
    _, parts, depth, rows, cols = wavefield.shape
    cell_count = parts * depth * rows * cols * lax.axis_size("space")
    f32, bf16 = jnp.float32, jnp.bfloat16
    anywhere = pl.BlockSpec(memory_space=pl.ANY)
    vmem = pl.BlockSpec(memory_space=pltpu.VMEM)
    smem = pl.BlockSpec(memory_space=pltpu.SMEM)
    dma = pltpu.SemaphoreType.DMA
    final, stored, sums = pl.pallas_call(
        kernel,
        out_shape=(
            jax.ShapeDtypeStruct(wavefield.shape, f32),
            jax.ShapeDtypeStruct((1, STEPS, parts, depth, rows, cols), bf16),
            jax.ShapeDtypeStruct((STEPS, 3, ROWS, cols), f32),
        ),
        in_specs=[anywhere] * 4 + [vmem, smem, smem],
        out_specs=(anywhere, anywhere, vmem),
        scratch_shapes=[
            pltpu.VMEM((2, parts, depth + 2 * REACH, rows + 2 * PAD, cols), f32),
            pltpu.VMEM((depth, rows, cols), f32),
            pltpu.VMEM((depth, rows, cols), f32),
            pltpu.VMEM((depth, rows, cols), f32),
            pltpu.VMEM((parts, rows, cols), f32),
            pltpu.VMEM((parts, rows, cols), f32),
            pltpu.VMEM((parts, depth, rows, cols), jnp.int16),
            pltpu.VMEM((parts, depth, rows, cols), jnp.int16),
            pltpu.VMEM((parts, ROWS, cols), f32),
            pltpu.VMEM((parts, ROWS, cols), f32),
            pltpu.VMEM((STEPS, parts, depth, rows, cols), bf16),
            pltpu.VMEM((2 * HALVES, 2, 5, rows, cols), bf16),
            pltpu.VMEM((2 * HALVES, 2, 5, rows, cols), bf16),
            dma((parts,)), dma((3,)), dma((parts,)), dma((STEPS,)),
            dma((parts,)), dma((parts,)), dma((parts,)), dma((parts,)),
            dma((2 * HALVES, 2)), dma((2 * HALVES, 2)),
        ],
        compiler_params=pltpu.CompilerParams(
            collective_id=0, has_side_effects=True, vmem_limit_bytes=48 * 1024 * 1024
        ),
        name="two_shots",
    )(wavefield, buoyancy, lame_lambda, shear_modulus, exponents[:, 0], cells, wavelet)
    totals = lax.psum(jnp.sum(sums, axis=(2, 3)), "space")
    mean_size = totals[:, 0] / cell_count
    relative = totals[:, 1] / cell_count / (totals[:, 2] / cell_count + FLOOR)
    statistics = jnp.stack([mean_size, jnp.sqrt(relative)], axis=-1)[None]
    return final, stored, statistics


def solution(mesh):
    return jax.shard_map(
        per_device,
        mesh=mesh,
        in_specs=(
            P("peer", None, "space", None, None),
            P("space", None, None),
            P("space", None, None),
            P("space", None, None),
            P(None, "space", None, None),
            P(),
            P(),
        ),
        out_specs=(
            P("peer", None, "space", None, None),
            P("peer", None, None, "space", None, None),
            P("peer", None, None),
        ),
        check_vma=False,
    )
```

```python
import functools

import jax
import jax.numpy as jnp
from jax import lax
from jax.experimental import pallas as pl
from jax.experimental.pallas import tpu as pltpu
from jax.sharding import PartitionSpec as P

BLOCK = 8
STEPS = 3
REACH = 2
W1, W2 = 9.0 / 8.0, -1.0 / 24.0
CLIP = 4.0
FLOOR = 1e-06
HALVES = 2 * STEPS
PAD = 8
ROWS = 16
LEVELS = 32700.0
TINY = 1e-30
MESH = pl.DeviceIdType.MESH

KINDS = {"stress": ((7, 8), (6,)), "velocity": ((2,), (0, 1))}
ARRIVAL = (6, 7, 8, 3, 5, 0, 4, 1, 2)


def rim_layers(kind, depth):
    back, ahead = KINDS[kind]
    up = [(c, depth - 2, -2) for c in back] + [(c, depth - 1, -1) for c in back + ahead]
    down = [(c, 0, depth) for c in back + ahead] + [(c, 1, depth + 1) for c in ahead]
    return up, down


def partner_of(slab, r):
    return slab + (1 << r) * (1 - 2 * ((slab // (1 << r)) % 2))


def kernel(
    wave, buoy_in, lam_in, mu_in, exps_in, cells, wavelet,
    final, stored, statistics,
    cur, buoy, lam, mu, up_t, down_t, tx, rx, unit_tx, unit_rx, pay, h_tx, h_rx, exps, sum_tx, sum_rx,
    load_sem, par_sem, out_sem, pay_sem, s_send, s_recv, u_send, u_recv, h_send, h_recv, r_send, r_recv,
):
    peer = lax.axis_index("peer")
    slab = lax.axis_index("space")
    count = lax.axis_size("space")
    depth, rows, cols = buoy.shape
    groups = rows // ROWS
    other = 1 - peer
    rounds = count.bit_length() - 1

    def body_of(shot, c):
        return cur.at[shot, c, pl.ds(REACH, depth), pl.ds(PAD, rows), :]

    loads = {}
    for c in ARRIVAL:
        loads[c] = pltpu.make_async_copy(wave.at[0, c], body_of(0, c), load_sem.at[c])
        loads[c].start()
    params = []
    for i, (src, dst) in enumerate(((buoy_in, buoy), (lam_in, lam), (mu_in, mu), (exps_in.at[:, 0], exps))):
        params.append(pltpu.make_async_copy(src, dst, par_sem.at[i]))
        params[-1].start()

    has_up = slab < count - 1
    has_down = slab > 0
    barrier = pltpu.get_barrier_semaphore()
    pl.semaphore_signal(barrier, inc=1, device_id={"peer": other}, device_id_type=MESH)

    @pl.when(has_up)
    def _():
        pl.semaphore_signal(barrier, inc=1, device_id={"space": slab + 1}, device_id_type=MESH)

    @pl.when(has_down)
    def _():
        pl.semaphore_signal(barrier, inc=1, device_id={"space": slab - 1}, device_id_type=MESH)

    for r in range(1, rounds):
        pl.semaphore_signal(
            barrier, inc=1, device_id={"space": partner_of(slab, r)}, device_id_type=MESH
        )

    edge_rows = jnp.zeros((PAD, cols), jnp.float32)
    edge_layer = jnp.zeros((rows, cols), jnp.float32)
    sum_tx[0] = jnp.zeros((ROWS, cols), jnp.float32)
    for shot in range(2):

        def clear(c, carry, shot=shot):
            for z in range(depth + 2 * REACH):
                cur[shot, c, z, pl.ds(0, PAD), :] = edge_rows
                cur[shot, c, z, pl.ds(PAD + rows, PAD), :] = edge_rows
            for z in (0, 1, depth + 2, depth + 3):
                cur[shot, c, z, pl.ds(PAD, rows), :] = edge_layer
            return carry

        lax.fori_loop(0, 9, clear, 0)

    neighbours = jnp.minimum(slab, 1) + jnp.minimum(count - 1 - slab, 1)
    pl.semaphore_wait(barrier, rounds + neighbours)

    def exchange(c):
        return pltpu.make_async_remote_copy(
            src_ref=tx.at[c], dst_ref=rx.at[c], send_sem=s_send.at[c], recv_sem=s_recv.at[c],
            device_id={"peer": other}, device_id_type=MESH,
        )

    def exchange_unit(c):
        return pltpu.make_async_remote_copy(
            src_ref=unit_tx.at[c], dst_ref=unit_rx.at[c], send_sem=u_send.at[c],
            recv_sem=u_recv.at[c], device_id={"peer": other}, device_id_type=MESH,
        )

    def halo(h, way, size):
        target = slab + 1 if way == 0 else slab - 1
        return pltpu.make_async_remote_copy(
            src_ref=h_tx.at[h, way, pl.ds(0, size)], dst_ref=h_rx.at[h, way, pl.ds(0, size)],
            send_sem=h_send.at[h, way], recv_sem=h_recv.at[h, way],
            device_id={"space": target}, device_id_type=MESH,
        )

    def send_rims(shot, kind, h):
        for way, layers in enumerate(rim_layers(kind, depth)):
            for i, (c, z, _) in enumerate(layers):
                h_tx[h, way, i] = cur[shot, c, REACH + z, pl.ds(PAD, rows), :].astype(jnp.bfloat16)

            @pl.when(has_up if way == 0 else has_down)
            def _():
                halo(h, way, len(layers)).start()

    def take_rims(shot, kind, h):
        for way, layers in enumerate(rim_layers(kind, depth)):

            @pl.when(has_down if way == 0 else has_up)
            def _():
                halo(h, way, len(layers)).wait_recv()
                for i, (c, _, z) in enumerate(layers):
                    cur[shot, c, REACH + z, pl.ds(PAD, rows), :] = h_rx[h, way, i].astype(
                        jnp.float32
                    )

    def finish_sends(kind, h):
        for way, layers in enumerate(rim_layers(kind, depth)):

            @pl.when(has_up if way == 0 else has_down)
            def _():
                halo(h, way, len(layers)).wait_send()

    lane = lax.broadcasted_iota(jnp.int32, (ROWS, cols), 1)
    row = lax.broadcasted_iota(jnp.int32, (ROWS, cols), 0)
    spot = row * cols + lane

    def shifted(f, k):
        moved = pltpu.roll(f, (-k) % cols, 1)
        keep = lane < cols - k if k > 0 else lane >= -k
        return jnp.where(keep, moved, 0.0)

    def along_x(f, ahead):
        if ahead:
            return W1 * (shifted(f, 1) - f) + W2 * (shifted(f, 2) - shifted(f, -1))
        return W1 * (f - shifted(f, -1)) + W2 * (shifted(f, 1) - shifted(f, -2))

    def reader(shot, z, g):
        base = PAD + g * ROWS

        def read(c, dz=0, dy=0):
            return cur[shot, c, z + (REACH + dz), pl.ds(base + dy, ROWS), :]

        def along_y(c, ahead):
            o = 1 if ahead else 0
            return W1 * (read(c, 0, o) - read(c, 0, o - 1)) + W2 * (
                read(c, 0, o + 1) - read(c, 0, o - 2)
            )

        def along_z(c, ahead):
            o = 1 if ahead else 0
            return W1 * (read(c, o) - read(c, o - 1)) + W2 * (read(c, o + 1) - read(c, o - 2))

        def write(c, value):
            cur[shot, c, z + REACH, pl.ds(base, ROWS), :] = value

        return read, along_y, along_z, write

    def velocity_layer(shot, z):
        for g in range(groups):
            read, along_y, along_z, write = reader(shot, z, g)
            b = buoy[z, pl.ds(g * ROWS, ROWS), :]
            write(0, read(0) + b * (along_x(read(3), True) + along_y(5, False) + along_z(7, False)))
            write(1, read(1) + b * (along_x(read(5), False) + along_y(4, True) + along_z(8, False)))
            write(2, read(2) + b * (along_x(read(7), False) + along_y(8, False) + along_z(6, True)))

    def stress_layer(shot, t, z, totals):
        shot_index = peer if shot == 0 else other
        for g in range(groups):
            read, along_y, along_z, write = reader(shot, z, g)
            part = pl.ds(g * ROWS, ROWS)
            vx, vy, vz = read(0), read(1), read(2)
            ex, ey, ez = along_x(vx, False), along_y(1, False), along_z(2, False)
            image = jnp.zeros((ROWS, cols), jnp.float32)
            start = ((slab * depth + z) * rows + g * ROWS) * cols
            for j in range(cells.shape[1]):
                image = image + jnp.where(
                    spot == cells[shot_index, j] - start, wavelet[t, shot_index, j], 0.0
                )
            m = mu[z, part, :]
            pressure = lam[z, part, :] * (ex + ey + ez) + image
            twice = 2.0 * m
            values = [
                vx, vy, vz,
                read(3) + pressure + twice * ex,
                read(4) + pressure + twice * ey,
                read(5) + m * (along_y(0, True) + along_x(vy, True)),
                read(6) + pressure + twice * ez,
                read(7) + m * (along_z(0, True) + along_x(vz, True)),
                read(8) + m * (along_z(1, True) + along_y(2, True)),
            ]
            for c in range(3, 9):
                write(c, values[c])
            for c in range(9):
                v = values[c]
                packed = jnp.clip(v * down_t[c, part, :], -CLIP, CLIP).astype(jnp.bfloat16)
                if shot == 1:
                    pay[t, c, z, part, :] = packed
                else:
                    level = packed.astype(jnp.float32)
                    miss = v - level * up_t[c, part, :]
                    totals = (
                        totals[0] + jnp.abs(level),
                        totals[1] + miss * miss,
                        totals[2] + v * v,
                    )
        return totals

    nothing = jnp.zeros((ROWS, cols), jnp.float32)

    def inner(k):
        return k + 2

    def outer(k):
        return jnp.where(k < 2, k, k + (depth - 4))

    def half(shot, i):
        t, h = i // 2, shot * HALVES + i
        kind = "stress" if i % 2 == 0 else "velocity"
        if i % 2 == 0:

            def run(place, size, totals):
                def step(k, carry):
                    velocity_layer(shot, place(k))
                    return carry

                lax.fori_loop(0, size, step, 0)
                return totals
        else:

            def run(place, size, totals):
                def step(k, carry):
                    return stress_layer(shot, t, place(k), carry)

                return lax.fori_loop(0, size, step, totals)

        totals = run(inner, depth - 4, (nothing,) * 3)
        take_rims(shot, kind, h)
        totals = run(outer, 4, totals)
        if i < HALVES - 1:
            send_rims(shot, "velocity" if i % 2 == 0 else "stress", h + 1)
        if i % 2 and shot == 0:
            for s in range(3):
                line = jnp.sum(totals[s], axis=0, keepdims=True)
                sum_tx[0, pl.ds(3 * t + s, 1), :] = line
        if i % 2 and shot == 1:
            payload_out(t).start()

    def payload_out(t):
        return pltpu.make_async_copy(pay.at[t], stored.at[0, t], pay_sem.at[t])

    def field_out(c):
        return pltpu.make_async_copy(body_of(0, c), final.at[0, c], out_sem.at[c])

    def swap_sums(r):
        return pltpu.make_async_remote_copy(
            src_ref=sum_tx.at[r], dst_ref=sum_rx.at[r], send_sem=r_send.at[r],
            recv_sem=r_recv.at[r], device_id={"space": partner_of(slab, r)}, device_id_type=MESH,
        )

    def add_sums(r):
        swap_sums(r).wait_recv()
        sum_tx[r + 1] = sum_tx[r] + sum_rx[r]
        if r + 1 < rounds:
            swap_sums(r + 1).start()

    def write_statistics():
        total = jnp.sum(sum_tx[rounds], axis=1, keepdims=True)
        cells_in_all = jnp.float32(9 * depth * rows * cols * count)
        at_row = lax.broadcasted_iota(jnp.int32, (STEPS, 2), 0)
        at_column = lax.broadcasted_iota(jnp.int32, (STEPS, 2), 1)
        result = jnp.zeros((STEPS, 2), jnp.float32)
        for t in range(STEPS):
            size, miss, power = (total[3 * t + s : 3 * t + s + 1] / cells_in_all for s in range(3))
            relative = jnp.sqrt(miss / (power + FLOOR))
            result = jnp.where(
                at_row == t, jnp.where(at_column == 0, size, relative), result
            )
        statistics[0] = result

    def unpack(c):
        exchange_unit(c).wait_recv()
        exchange(c).wait_recv()
        unit = unit_rx[c]

        def step(z, carry):
            for g in range(groups):
                whole = rx[c, z, pl.ds(g * ROWS, ROWS), :].astype(jnp.int32)
                cur[1, c, z + REACH, pl.ds(PAD + g * ROWS, ROWS), :] = (
                    whole.astype(jnp.float32) * unit
                )
            return carry

        lax.fori_loop(0, depth, step, 0)

    for c in ARRIVAL:
        loads[c].wait()

        def largest(z, top, c=c):
            for g in range(groups):
                top = jnp.maximum(
                    top, jnp.abs(cur[0, c, z + REACH, pl.ds(PAD + g * ROWS, ROWS), :])
                )
            return top

        top = lax.fori_loop(0, depth, largest, jnp.full((ROWS, cols), TINY, jnp.float32))
        unit_tx[c] = top * (1.0 / LEVELS)
        inverse = LEVELS / top

        def pack(z, carry, c=c, inverse=inverse):
            for g in range(groups):
                value = cur[0, c, z + REACH, pl.ds(PAD + g * ROWS, ROWS), :] * inverse
                tx[c, z, pl.ds(g * ROWS, ROWS), :] = (
                    jnp.round(value).astype(jnp.int32).astype(jnp.int16)
                )
            return carry

        lax.fori_loop(0, depth, pack, 0)
        exchange_unit(c).start()
        exchange(c).start()
        if c == 8:
            send_rims(0, "stress", 0)

    bands, strips = exps.shape[1], exps.shape[2]
    spread_y = (
        lax.broadcasted_iota(jnp.int32, (rows, bands), 0) // BLOCK
        == lax.broadcasted_iota(jnp.int32, (rows, bands), 1)
    ).astype(jnp.float32)
    spread_x = (
        lax.broadcasted_iota(jnp.int32, (strips, cols), 1) // BLOCK
        == lax.broadcasted_iota(jnp.int32, (strips, cols), 0)
    ).astype(jnp.float32)
    params.pop().wait()
    for c in range(9):
        e = exps[c]
        for table, sign in ((up_t, 1), (down_t, -1)):
            scale = jnp.zeros(e.shape, jnp.float32)
            for power in range(-2, 3):
                scale = jnp.where(e == power, jnp.float32(2.0 ** (sign * power)), scale)
            wide = jnp.dot(scale, spread_x, preferred_element_type=jnp.float32)
            table[c] = jnp.dot(spread_y, wide, preferred_element_type=jnp.float32)

    for p in params:
        p.wait()
    half(0, 0)
    half(0, 1)
    half(0, 2)
    for c in ARRIVAL[:3]:
        unpack(c)
    send_rims(1, "stress", HALVES)
    half(0, 3)
    for c in ARRIVAL[3:]:
        unpack(c)
    half(1, 0)
    half(0, 4)
    half(1, 1)
    half(0, 5)
    swap_sums(0).start()
    for c in range(9):
        field_out(c).start()
    done = 0
    for i in range(2, HALVES):
        half(1, i)
        if done < rounds:
            add_sums(done)
            done += 1
    for r in range(done, rounds):
        add_sums(r)
    write_statistics()
    for r in range(rounds):
        swap_sums(r).wait_send()

    for c in ARRIVAL:
        exchange(c).wait_send()
        exchange_unit(c).wait_send()
    for shot in range(2):
        for i in range(HALVES):
            finish_sends("stress" if i % 2 == 0 else "velocity", shot * HALVES + i)
    for c in range(9):
        field_out(c).wait()
    for t in range(STEPS):
        payload_out(t).wait()


def per_device(wavefield, buoyancy, lame_lambda, shear_modulus, exponents, cells, wavelet):
    _, parts, depth, rows, cols = wavefield.shape
    rounds = lax.axis_size("space").bit_length() - 1
    f32, bf16 = jnp.float32, jnp.bfloat16
    anywhere = pl.BlockSpec(memory_space=pl.ANY)
    vmem = pl.BlockSpec(memory_space=pltpu.VMEM)
    smem = pl.BlockSpec(memory_space=pltpu.SMEM)
    dma = pltpu.SemaphoreType.DMA
    return pl.pallas_call(
        kernel,
        out_shape=(
            jax.ShapeDtypeStruct(wavefield.shape, f32),
            jax.ShapeDtypeStruct((1, STEPS, parts, depth, rows, cols), bf16),
            jax.ShapeDtypeStruct((1, STEPS, 2), f32),
        ),
        in_specs=[anywhere] * 5 + [smem, smem],
        out_specs=(anywhere, anywhere, vmem),
        scratch_shapes=[
            pltpu.VMEM((2, parts, depth + 2 * REACH, rows + 2 * PAD, cols), f32),
            pltpu.VMEM((depth, rows, cols), f32),
            pltpu.VMEM((depth, rows, cols), f32),
            pltpu.VMEM((depth, rows, cols), f32),
            pltpu.VMEM((parts, rows, cols), f32),
            pltpu.VMEM((parts, rows, cols), f32),
            pltpu.VMEM((parts, depth, rows, cols), jnp.int16),
            pltpu.VMEM((parts, depth, rows, cols), jnp.int16),
            pltpu.VMEM((parts, ROWS, cols), f32),
            pltpu.VMEM((parts, ROWS, cols), f32),
            pltpu.VMEM((STEPS, parts, depth, rows, cols), bf16),
            pltpu.VMEM((2 * HALVES, 2, 5, rows, cols), bf16),
            pltpu.VMEM((2 * HALVES, 2, 5, rows, cols), bf16),
            pltpu.VMEM((parts,) + exponents.shape[2:], jnp.int32),
            pltpu.VMEM((rounds + 1, ROWS, cols), f32),
            pltpu.VMEM((rounds, ROWS, cols), f32),
            dma((parts,)), dma((4,)), dma((parts,)), dma((STEPS,)),
            dma((parts,)), dma((parts,)), dma((parts,)), dma((parts,)),
            dma((2 * HALVES, 2)), dma((2 * HALVES, 2)), dma((rounds,)), dma((rounds,)),
        ],
        compiler_params=pltpu.CompilerParams(
            collective_id=0, has_side_effects=True, vmem_limit_bytes=67043328
        ),
        name="two_shots",
    )(wavefield, buoyancy, lame_lambda, shear_modulus, exponents, cells, wavelet.transpose(1, 0, 2))


def solution(mesh):
    return jax.shard_map(
        per_device,
        mesh=mesh,
        in_specs=(
            P("peer", None, "space", None, None),
            P("space", None, None),
            P("space", None, None),
            P("space", None, None),
            P(None, "space", None, None),
            P(),
            P(),
        ),
        out_specs=(
            P("peer", None, "space", None, None),
            P("peer", None, None, "space", None, None),
            P("peer", None, None),
        ),
        check_vma=False,
    )
```

```python
import functools

import jax
import jax.numpy as jnp
from jax import lax
from jax.experimental import pallas as pl
from jax.experimental.pallas import tpu as pltpu
from jax.sharding import PartitionSpec as P

BLOCK = 8
STEPS = 3
REACH = 2
W1, W2 = 9.0 / 8.0, -1.0 / 24.0
CLIP = 4.0
FLOOR = 1e-06
HALVES = 2 * STEPS
PAD = 8
ROWS = 16
HANDED = 2
LEVELS = 32700.0
TINY = 1e-30
MESH = pl.DeviceIdType.MESH

KINDS = {"stress": ((7, 8), (6,)), "velocity": ((2,), (0, 1))}
ARRIVAL = (6, 7, 8, 3, 5, 0, 4, 1, 2)


def rim_layers(kind, depth):
    back, ahead = KINDS[kind]
    up = [(c, depth - 2, -2) for c in back] + [(c, depth - 1, -1) for c in back + ahead]
    down = [(c, 0, depth) for c in back + ahead] + [(c, 1, depth + 1) for c in ahead]
    return up, down


def partner_of(slab, r):
    return slab + (1 << r) * (1 - 2 * ((slab // (1 << r)) % 2))


def kernel(
    wave, buoy_in, lam_in, mu_in, exps_in, cells, wavelet,
    final, stored, statistics,
    cur, buoy, lam, mu, up_t, down_t, tx, rx, unit_tx, unit_rx, pay, h_tx, h_rx, exps, sum_tx, sum_rx,
    load_sem, par_sem, out_sem, pay_sem, s_send, s_recv, u_send, u_recv, h_send, h_recv, f_send, f_recv, r_send, r_recv,
):
    peer = lax.axis_index("peer")
    slab = lax.axis_index("space")
    count = lax.axis_size("space")
    depth, rows, cols = buoy.shape
    groups = rows // ROWS
    other = 1 - peer
    rounds = count.bit_length() - 1

    def body_of(shot, c):
        return cur.at[shot, c, pl.ds(REACH, depth), pl.ds(PAD, rows), :]

    loads = {}
    for c in ARRIVAL:
        loads[c] = pltpu.make_async_copy(wave.at[0, c], body_of(0, c), load_sem.at[c])
        loads[c].start()
    params = []
    for i, (src, dst) in enumerate(((buoy_in, buoy), (lam_in, lam), (mu_in, mu), (exps_in.at[:, 0], exps))):
        params.append(pltpu.make_async_copy(src, dst, par_sem.at[i]))
        params[-1].start()

    has_up = slab < count - 1
    has_down = slab > 0
    barrier = pltpu.get_barrier_semaphore()
    pl.semaphore_signal(barrier, inc=1, device_id={"peer": other}, device_id_type=MESH)

    @pl.when(has_up)
    def _():
        pl.semaphore_signal(barrier, inc=1, device_id={"space": slab + 1}, device_id_type=MESH)

    @pl.when(has_down)
    def _():
        pl.semaphore_signal(barrier, inc=1, device_id={"space": slab - 1}, device_id_type=MESH)

    for r in range(1, rounds):
        pl.semaphore_signal(
            barrier, inc=1, device_id={"space": partner_of(slab, r)}, device_id_type=MESH
        )

    edge_rows = jnp.zeros((PAD, cols), jnp.float32)
    edge_layer = jnp.zeros((rows, cols), jnp.float32)
    sum_tx[0] = jnp.zeros((ROWS, cols), jnp.float32)
    for shot in range(2):

        def clear(c, carry, shot=shot):
            for z in range(depth + 2 * REACH):
                cur[shot, c, z, pl.ds(0, PAD), :] = edge_rows
                cur[shot, c, z, pl.ds(PAD + rows, PAD), :] = edge_rows
            for z in (0, 1, depth + 2, depth + 3):
                cur[shot, c, z, pl.ds(PAD, rows), :] = edge_layer
            return carry

        lax.fori_loop(0, 9, clear, 0)

    neighbours = jnp.minimum(slab, 1) + jnp.minimum(count - 1 - slab, 1)
    pl.semaphore_wait(barrier, rounds + neighbours)

    def exchange(c):
        return pltpu.make_async_remote_copy(
            src_ref=tx.at[c], dst_ref=rx.at[c], send_sem=s_send.at[c], recv_sem=s_recv.at[c],
            device_id={"peer": other}, device_id_type=MESH,
        )

    def exchange_unit(c):
        return pltpu.make_async_remote_copy(
            src_ref=unit_tx.at[c], dst_ref=unit_rx.at[c], send_sem=u_send.at[c],
            recv_sem=u_recv.at[c], device_id={"peer": other}, device_id_type=MESH,
        )

    def halo(h, way, size):
        target = slab + 1 if way == 0 else slab - 1
        return pltpu.make_async_remote_copy(
            src_ref=h_tx.at[h, way, pl.ds(0, size)], dst_ref=h_rx.at[h, way, pl.ds(0, size)],
            send_sem=h_send.at[h, way], recv_sem=h_recv.at[h, way],
            device_id={"space": target}, device_id_type=MESH,
        )

    def handed(i, way, size):
        return pltpu.make_async_remote_copy(
            src_ref=h_rx.at[i, way, pl.ds(0, size)],
            dst_ref=h_rx.at[HALVES + i, way, pl.ds(0, size)],
            send_sem=f_send.at[i, way], recv_sem=f_recv.at[i, way],
            device_id={"peer": other}, device_id_type=MESH,
        )

    def send_rims(shot, kind, h):
        for way, layers in enumerate(rim_layers(kind, depth)):
            for i, (c, z, _) in enumerate(layers):
                h_tx[h, way, i] = cur[shot, c, REACH + z, pl.ds(PAD, rows), :].astype(jnp.bfloat16)

            @pl.when(has_up if way == 0 else has_down)
            def _():
                halo(h, way, len(layers)).start()

    def take_rims(shot, kind, h):
        for way, layers in enumerate(rim_layers(kind, depth)):

            @pl.when(has_down if way == 0 else has_up)
            def _():
                if shot == 1 and h - HALVES >= HANDED:
                    handed(h - HALVES, way, len(layers)).wait_recv()
                else:
                    halo(h, way, len(layers)).wait_recv()
                if shot == 0 and h >= HANDED:
                    handed(h, way, len(layers)).start()
                for i, (c, _, z) in enumerate(layers):
                    cur[shot, c, REACH + z, pl.ds(PAD, rows), :] = h_rx[h, way, i].astype(
                        jnp.float32
                    )

    def finish_sends(kind, h):
        for way, layers in enumerate(rim_layers(kind, depth)):

            @pl.when(has_up if way == 0 else has_down)
            def _():
                halo(h, way, len(layers)).wait_send()

    def finish_handed(kind, i):
        for way, layers in enumerate(rim_layers(kind, depth)):

            @pl.when(has_down if way == 0 else has_up)
            def _():
                handed(i, way, len(layers)).wait_send()

    lane = lax.broadcasted_iota(jnp.int32, (ROWS, cols), 1)
    row = lax.broadcasted_iota(jnp.int32, (ROWS, cols), 0)
    spot = row * cols + lane

    def shifted(f, k):
        moved = pltpu.roll(f, (-k) % cols, 1)
        keep = lane < cols - k if k > 0 else lane >= -k
        return jnp.where(keep, moved, 0.0)

    def along_x(f, ahead):
        if ahead:
            return W1 * (shifted(f, 1) - f) + W2 * (shifted(f, 2) - shifted(f, -1))
        return W1 * (f - shifted(f, -1)) + W2 * (shifted(f, 1) - shifted(f, -2))

    def reader(shot, z, g):
        base = PAD + g * ROWS

        def read(c, dz=0, dy=0):
            return cur[shot, c, z + (REACH + dz), pl.ds(base + dy, ROWS), :]

        def along_y(c, ahead):
            o = 1 if ahead else 0
            return W1 * (read(c, 0, o) - read(c, 0, o - 1)) + W2 * (
                read(c, 0, o + 1) - read(c, 0, o - 2)
            )

        def along_z(c, ahead):
            o = 1 if ahead else 0
            return W1 * (read(c, o) - read(c, o - 1)) + W2 * (read(c, o + 1) - read(c, o - 2))

        def write(c, value):
            cur[shot, c, z + REACH, pl.ds(base, ROWS), :] = value

        return read, along_y, along_z, write

    def velocity_layer(shot, z):
        for g in range(groups):
            read, along_y, along_z, write = reader(shot, z, g)
            b = buoy[z, pl.ds(g * ROWS, ROWS), :]
            write(0, read(0) + b * (along_x(read(3), True) + along_y(5, False) + along_z(7, False)))
            write(1, read(1) + b * (along_x(read(5), False) + along_y(4, True) + along_z(8, False)))
            write(2, read(2) + b * (along_x(read(7), False) + along_y(8, False) + along_z(6, True)))

    def stress_layer(shot, t, z, totals):
        shot_index = peer if shot == 0 else other
        for g in range(groups):
            read, along_y, along_z, write = reader(shot, z, g)
            part = pl.ds(g * ROWS, ROWS)
            vx, vy, vz = read(0), read(1), read(2)
            ex, ey, ez = along_x(vx, False), along_y(1, False), along_z(2, False)
            image = jnp.zeros((ROWS, cols), jnp.float32)
            start = ((slab * depth + z) * rows + g * ROWS) * cols
            for j in range(cells.shape[1]):
                image = image + jnp.where(
                    spot == cells[shot_index, j] - start, wavelet[t, shot_index, j], 0.0
                )
            m = mu[z, part, :]
            pressure = lam[z, part, :] * (ex + ey + ez) + image
            twice = 2.0 * m
            values = [
                vx, vy, vz,
                read(3) + pressure + twice * ex,
                read(4) + pressure + twice * ey,
                read(5) + m * (along_y(0, True) + along_x(vy, True)),
                read(6) + pressure + twice * ez,
                read(7) + m * (along_z(0, True) + along_x(vz, True)),
                read(8) + m * (along_z(1, True) + along_y(2, True)),
            ]
            for c in range(3, 9):
                write(c, values[c])
            for c in range(9):
                v = values[c]
                packed = jnp.clip(v * down_t[c, part, :], -CLIP, CLIP).astype(jnp.bfloat16)
                if shot == 1:
                    pay[t, c, z, part, :] = packed
                else:
                    level = packed.astype(jnp.float32)
                    miss = v - level * up_t[c, part, :]
                    totals = (
                        totals[0] + jnp.abs(level),
                        totals[1] + miss * miss,
                        totals[2] + v * v,
                    )
        return totals

    nothing = jnp.zeros((ROWS, cols), jnp.float32)

    def inner(k):
        return k + 2

    def outer(k):
        return jnp.where(k < 2, k, k + (depth - 4))

    def half(shot, i):
        t, h = i // 2, shot * HALVES + i
        kind = "stress" if i % 2 == 0 else "velocity"
        if i % 2 == 0:

            def run(place, size, totals):
                def step(k, carry):
                    velocity_layer(shot, place(k))
                    return carry

                lax.fori_loop(0, size, step, 0)
                return totals
        else:

            def run(place, size, totals):
                def step(k, carry):
                    return stress_layer(shot, t, place(k), carry)

                return lax.fori_loop(0, size, step, totals)

        totals = run(inner, depth - 4, (nothing,) * 3)
        take_rims(shot, kind, h)
        totals = run(outer, 4, totals)
        if i < HALVES - 1 and (shot == 0 or i + 1 < HANDED):
            send_rims(shot, "velocity" if i % 2 == 0 else "stress", h + 1)
        if i % 2 and shot == 0:
            for s in range(3):
                line = jnp.sum(totals[s], axis=0, keepdims=True)
                sum_tx[0, pl.ds(3 * t + s, 1), :] = line
        if i % 2 and shot == 1:
            payload_out(t).start()

    def payload_out(t):
        return pltpu.make_async_copy(pay.at[t], stored.at[0, t], pay_sem.at[t])

    def field_out(c):
        return pltpu.make_async_copy(body_of(0, c), final.at[0, c], out_sem.at[c])

    def swap_sums(r):
        return pltpu.make_async_remote_copy(
            src_ref=sum_tx.at[r], dst_ref=sum_rx.at[r], send_sem=r_send.at[r],
            recv_sem=r_recv.at[r], device_id={"space": partner_of(slab, r)}, device_id_type=MESH,
        )

    def add_sums(r):
        swap_sums(r).wait_recv()
        sum_tx[r + 1] = sum_tx[r] + sum_rx[r]
        if r + 1 < rounds:
            swap_sums(r + 1).start()

    def write_statistics():
        total = jnp.sum(sum_tx[rounds], axis=1, keepdims=True)
        cells_in_all = jnp.float32(9 * depth * rows * cols * count)
        at_row = lax.broadcasted_iota(jnp.int32, (STEPS, 2), 0)
        at_column = lax.broadcasted_iota(jnp.int32, (STEPS, 2), 1)
        result = jnp.zeros((STEPS, 2), jnp.float32)
        for t in range(STEPS):
            size, miss, power = (total[3 * t + s : 3 * t + s + 1] / cells_in_all for s in range(3))
            relative = jnp.sqrt(miss / (power + FLOOR))
            result = jnp.where(
                at_row == t, jnp.where(at_column == 0, size, relative), result
            )
        statistics[0] = result

    def unpack(c):
        exchange_unit(c).wait_recv()
        exchange(c).wait_recv()
        unit = unit_rx[c]

        def step(z, carry):
            for g in range(groups):
                whole = rx[c, z, pl.ds(g * ROWS, ROWS), :].astype(jnp.int32)
                cur[1, c, z + REACH, pl.ds(PAD + g * ROWS, ROWS), :] = (
                    whole.astype(jnp.float32) * unit
                )
            return carry

        lax.fori_loop(0, depth, step, 0)

    for c in ARRIVAL:
        loads[c].wait()

        def largest(z, top, c=c):
            for g in range(groups):
                top = jnp.maximum(
                    top, jnp.abs(cur[0, c, z + REACH, pl.ds(PAD + g * ROWS, ROWS), :])
                )
            return top

        top = lax.fori_loop(0, depth, largest, jnp.full((ROWS, cols), TINY, jnp.float32))
        unit_tx[c] = top * (1.0 / LEVELS)
        inverse = LEVELS / top

        def pack(z, carry, c=c, inverse=inverse):
            for g in range(groups):
                value = cur[0, c, z + REACH, pl.ds(PAD + g * ROWS, ROWS), :] * inverse
                tx[c, z, pl.ds(g * ROWS, ROWS), :] = (
                    jnp.round(value).astype(jnp.int32).astype(jnp.int16)
                )
            return carry

        lax.fori_loop(0, depth, pack, 0)
        exchange_unit(c).start()
        exchange(c).start()
        if c == 8:
            send_rims(0, "stress", 0)

    bands, strips = exps.shape[1], exps.shape[2]
    spread_y = (
        lax.broadcasted_iota(jnp.int32, (rows, bands), 0) // BLOCK
        == lax.broadcasted_iota(jnp.int32, (rows, bands), 1)
    ).astype(jnp.float32)
    spread_x = (
        lax.broadcasted_iota(jnp.int32, (strips, cols), 1) // BLOCK
        == lax.broadcasted_iota(jnp.int32, (strips, cols), 0)
    ).astype(jnp.float32)
    params.pop().wait()
    for c in range(9):
        e = exps[c]
        for table, sign in ((up_t, 1), (down_t, -1)):
            scale = jnp.zeros(e.shape, jnp.float32)
            for power in range(-2, 3):
                scale = jnp.where(e == power, jnp.float32(2.0 ** (sign * power)), scale)
            wide = jnp.dot(scale, spread_x, preferred_element_type=jnp.float32)
            table[c] = jnp.dot(spread_y, wide, preferred_element_type=jnp.float32)

    for p in params:
        p.wait()
    half(0, 0)
    half(0, 1)
    half(0, 2)
    for c in ARRIVAL[:3]:
        unpack(c)
    send_rims(1, "stress", HALVES)
    half(0, 3)
    for c in ARRIVAL[3:]:
        unpack(c)
    half(1, 0)
    half(0, 4)
    half(1, 1)
    half(0, 5)
    swap_sums(0).start()
    for c in range(9):
        field_out(c).start()
    done = 0
    for i in range(2, HALVES):
        half(1, i)
        if done < rounds:
            add_sums(done)
            done += 1
    for r in range(done, rounds):
        add_sums(r)
    write_statistics()
    for r in range(rounds):
        swap_sums(r).wait_send()

    for c in ARRIVAL:
        exchange(c).wait_send()
        exchange_unit(c).wait_send()
    for shot in range(2):
        for i in range(HALVES):
            kind = "stress" if i % 2 == 0 else "velocity"
            if shot == 0 or i < HANDED:
                finish_sends(kind, shot * HALVES + i)
            else:
                finish_handed(kind, i)
    for c in range(9):
        field_out(c).wait()
    for t in range(STEPS):
        payload_out(t).wait()


def per_device(wavefield, buoyancy, lame_lambda, shear_modulus, exponents, cells, wavelet):
    _, parts, depth, rows, cols = wavefield.shape
    rounds = lax.axis_size("space").bit_length() - 1
    f32, bf16 = jnp.float32, jnp.bfloat16
    anywhere = pl.BlockSpec(memory_space=pl.ANY)
    vmem = pl.BlockSpec(memory_space=pltpu.VMEM)
    smem = pl.BlockSpec(memory_space=pltpu.SMEM)
    dma = pltpu.SemaphoreType.DMA
    return pl.pallas_call(
        kernel,
        out_shape=(
            jax.ShapeDtypeStruct(wavefield.shape, f32),
            jax.ShapeDtypeStruct((1, STEPS, parts, depth, rows, cols), bf16),
            jax.ShapeDtypeStruct((1, STEPS, 2), f32),
        ),
        in_specs=[anywhere] * 5 + [smem, smem],
        out_specs=(anywhere, anywhere, vmem),
        scratch_shapes=[
            pltpu.VMEM((2, parts, depth + 2 * REACH, rows + 2 * PAD, cols), f32),
            pltpu.VMEM((depth, rows, cols), f32),
            pltpu.VMEM((depth, rows, cols), f32),
            pltpu.VMEM((depth, rows, cols), f32),
            pltpu.VMEM((parts, rows, cols), f32),
            pltpu.VMEM((parts, rows, cols), f32),
            pltpu.VMEM((parts, depth, rows, cols), jnp.int16),
            pltpu.VMEM((parts, depth, rows, cols), jnp.int16),
            pltpu.VMEM((parts, ROWS, cols), f32),
            pltpu.VMEM((parts, ROWS, cols), f32),
            pltpu.VMEM((STEPS, parts, depth, rows, cols), bf16),
            pltpu.VMEM((2 * HALVES, 2, 5, rows, cols), bf16),
            pltpu.VMEM((2 * HALVES, 2, 5, rows, cols), bf16),
            pltpu.VMEM((parts,) + exponents.shape[2:], jnp.int32),
            pltpu.VMEM((rounds + 1, ROWS, cols), f32),
            pltpu.VMEM((rounds, ROWS, cols), f32),
            dma((parts,)), dma((4,)), dma((parts,)), dma((STEPS,)),
            dma((parts,)), dma((parts,)), dma((parts,)), dma((parts,)),
            dma((2 * HALVES, 2)), dma((2 * HALVES, 2)),
            dma((HALVES, 2)), dma((HALVES, 2)), dma((rounds,)), dma((rounds,)),
        ],
        compiler_params=pltpu.CompilerParams(
            collective_id=0, has_side_effects=True, vmem_limit_bytes=67043328
        ),
        name="two_shots",
    )(wavefield, buoyancy, lame_lambda, shear_modulus, exponents, cells, wavelet.transpose(1, 0, 2))


def solution(mesh):
    return jax.shard_map(
        per_device,
        mesh=mesh,
        in_specs=(
            P("peer", None, "space", None, None),
            P("space", None, None),
            P("space", None, None),
            P("space", None, None),
            P(None, "space", None, None),
            P(),
            P(),
        ),
        out_specs=(
            P("peer", None, "space", None, None),
            P("peer", None, None, "space", None, None),
            P("peer", None, None),
        ),
        check_vma=False,
    )
```
